32 devices in a mesh: slab: 4 (over z), swap: 8 (over y, x, core).
Axes of the slice: x: 2, y: 2, z: 4, core: 2. Of those that a mesh axis runs over, the one named last changes fastest.
Arguments:
- fluid_state: float32 [2, 128, 128, 256], P(None, ('slab', 'swap')), may hold values from -0.45 to 1.6, as said below
- material: int32 [128, 128, 256], P(('slab', 'swap')), may hold values from 0 to 7
- table_colour: float32 [3, 8], replicated, may hold values from 0.2 to 2
- table_extinction: float32 [8], replicated, may hold values from 0.2 to 1.5
Outputs:
- new_density: float32 [128, 128, 256], P(('slab', 'swap'))
- rendered: float32 [4, 32768], P(None, 'swap')
The draws below stay inside these ranges and needn't reach their ends.
Inputs may be any that keep to these rules, and one draw needn't show every extreme that they name: fluid_state[0] is the density, between 0.6 and 1.6; fluid_state[1] is the momentum along the view axis, between -0.45 and 0.45.
All inputs are finite; a program needn't handle non-finite values.
Results may differ from the reference program's by a relative error of at most 0.0003.
Values sent between devices are 32-bit elements; how exact they have to be, the bound alone decides.
No kernel may reach another device: no remote copies, remote signals or barrier semaphores. Data moves between devices by JAX's collectives and lax.ppermute only.
A program may use at most 64 MiB of HBM per device.

```python
import math
import jax
import jax.numpy as jnp

NX = 128
NY = 256
MATERIALS = 8
NZ = 128


def draw_fluid_state(key, part):
    first_key, second_key = jax.random.split(jax.random.fold_in(key, 11))
    extent = (NZ, NX, NY)
    density = jnp.exp(jax.random.uniform(first_key, extent, jnp.float32, math.log(0.6), math.log(1.6)))
    momentum = jax.random.uniform(second_key, extent, jnp.float32, -0.45, 0.45)
    return jnp.stack([density, momentum]).astype(jnp.float32)


def place_ends(array, key, low, top_value):
    shape = array.shape
    place = [jax.random.randint(jax.random.fold_in(key, axis), (), 0, shape[axis]) for axis in range(len(shape))]
    array = array.at[tuple(place)].set(low)
    longest = shape.index(max(shape))
    place[longest] = (place[longest] + 1) % shape[longest]
    return array.at[tuple(place)].set(top_value)


def setup_inputs(seed: int = 0) -> dict:
    splits = jax.random.split(jax.random.key(seed), 5)
    return {
        "fluid_state": draw_fluid_state(jax.random.fold_in(splits[4], 71), 0),
        "material": place_ends(jax.random.randint(splits[1], (NZ, NX, NY), 0, MATERIALS), jax.random.fold_in(splits[1], 1), 0, MATERIALS - 1).astype(jnp.int32),
        "table_colour": jnp.clip(jax.random.uniform(splits[2], (3, MATERIALS), jnp.float32, 0.2, 2.0), 0.2, 2.0),
        "table_extinction": jnp.clip(jnp.exp(jax.random.uniform(splits[3], (MATERIALS,), jnp.float32, math.log(0.2), math.log(1.5))), 0.2, 1.5),
    }


COURANT = 0.4
DEPTH_SCALE = 2.5


def hydro_step(fields):
    density = fields[0]
    momentum = fields[1]
    velocity = momentum / density
    speeds = jnp.abs(velocity) + 1.0
    fluxes = jnp.stack([momentum, momentum * velocity + density])
    face_speed = jnp.maximum(speeds[:-1], speeds[1:])
    face_flux = 0.5 * (fluxes[:, :-1] + fluxes[:, 1:]) - 0.5 * face_speed * (fields[:, 1:] - fields[:, :-1])
    return fields[:, 1:-1] - COURANT * (face_flux[:, 1:] - face_flux[:, :-1])


def reference(fluid_state, material, table_colour, table_extinction):
    fields = fluid_state
    for number in range(4):
        padded = jnp.concatenate([fields[:, -1:], fields, fields[:, :1]], axis=1)
        fields = hydro_step(padded)
    density = fields[0]
    extinction = jnp.zeros(density.shape, jnp.float32)
    for number in range(MATERIALS):
        extinction = extinction + jnp.where(material == number, table_extinction[number], 0.0)
    optical = DEPTH_SCALE * extinction * density / NZ
    running = jnp.cumsum(optical, axis=0)
    weight = jnp.exp(optical - running) * (1.0 - jnp.exp(-optical))
    colour = jnp.zeros((3, NX, NY), jnp.float32)
    for number in range(MATERIALS):
        summed = jnp.sum(jnp.where(material == number, weight, 0.0), axis=0)
        colour = colour + table_colour[:, number][:, None, None] * summed[None]
    opacity = 1.0 - jnp.exp(-running[-1])
    rendered = jnp.concatenate([colour, opacity[None]], axis=0).reshape(4, NX * NY)
    return density, rendered
```

```python
import functools

import jax
import jax.numpy as jnp
from jax import lax
from jax.experimental import pallas as pl
from jax.experimental.pallas import tpu as pltpu
from jax.sharding import PartitionSpec as P

COURANT = 0.4
DEPTH_SCALE = 2.5
LANES = 128
VMEM = pl.BlockSpec(memory_space=pltpu.VMEM)


def routes(members):
    half = members // 2
    return [[(w, 2 * ((w % half) ^ r) + w // half) for w in range(members)] for r in range(half)]


def pick(arrays, index):
    out = arrays[0]
    for number in range(1, len(arrays)):
        out = jnp.where(index == number, arrays[number], out)
    return out


def advance(state, stage, density, momentum, emit):
    if stage == 4:
        emit(density)
        return
    last = stage == 3
    velocity = momentum / density
    speed = jnp.abs(velocity) + 1.0
    pressure = None if last else momentum * velocity + density
    held = state[stage]
    if held is None:
        state[stage] = (density, momentum, speed, pressure, None, None)
        return
    density0, momentum0, speed0, pressure0, mass0, force0 = held
    face = jnp.maximum(speed0, speed)
    mass = (momentum0 + momentum) - face * (density - density0)
    force = None if last else (pressure0 + pressure) - face * (momentum - momentum0)
    state[stage] = (density, momentum, speed, pressure, mass, force)
    if mass0 is None:
        return
    density1 = density0 - (0.5 * COURANT) * (mass - mass0)
    momentum1 = None if last else momentum0 - (0.5 * COURANT) * (force - force0)
    advance(state, stage + 1, density1, momentum1, emit)


def sweep_kernel(half, *refs):
    blocks, materials = refs[:half], refs[half : 2 * half]
    near, far, table = refs[2 * half : 2 * half + 3]
    density_out = refs[2 * half + 3 : 3 * half + 3]
    image, fluid, kind, dense = refs[3 * half + 3 :]
    member = lax.axis_index("swap")
    chip, upper = member // 2, member % 2
    layers, rows, columns = blocks[0].shape[1:]
    for r in range(half):
        fluid[:, pl.ds((1 + (chip ^ r)) * layers, layers)] = blocks[r][...]
        kind[pl.ds((chip ^ r) * layers, layers)] = materials[r][...]
    near_at = jnp.where(upper == 1, 0, half + 1)
    far_at = jnp.where(upper == 1, half + 1, 0)
    fluid[:, pl.ds(near_at * layers, layers)] = near[...]
    fluid[:, pl.ds(far_at * layers, layers)] = far[...]

    tall = min(8, rows)
    across = columns // LANES

    def tile(number, carry):
        row = pl.ds(pl.multiple_of(number // across * tall, tall), tall)
        column = pl.ds(pl.multiple_of(number % across * LANES, LANES), LANES)

        def block(state, light, position):
            for layer in range(layers):
                at = position * layers + layer

                def emit(density):
                    own = at - 2 * layers
                    dense[own, row, column] = density
                    which = kind[own, row, column]
                    factor, red, green, blue = (
                        jnp.take_along_axis(table[n, :tall, :], which, axis=1) for n in range(4)
                    )
                    through = jnp.exp(-(factor * density))
                    weight = light[0] * (1.0 - through)
                    light[0] = light[0] * through
                    light[1] = light[1] + weight * red
                    light[2] = light[2] + weight * green
                    light[3] = light[3] + weight * blue

                advance(state, 0, fluid[0, at, row, column], fluid[1, at, row, column], emit)

        state = [None] * 4
        zero = jnp.zeros((tall, LANES), jnp.float32)
        light = [zero + 1.0, zero, zero, zero]
        block(state, light, 0)
        block(state, light, 1)
        if half <= 4:
            for position in range(2, half + 2):
                block(state, light, position)
        else:

            def step(position, carry):
                state, light = [list(part) for part in carry]
                state = [tuple(held) for held in state]
                block(state, light, position)
                return state, light

            state, light = lax.fori_loop(2, half + 2, step, (state, light))
        image[0, row, column] = light[1]
        image[1, row, column] = light[2]
        image[2, row, column] = light[3]
        image[3, row, column] = 1.0 - light[0]
        return carry

    lax.fori_loop(0, rows // tall * across, tile, 0)
    for r in range(half):
        density_out[r][...] = dense[pl.ds((chip ^ r) * layers, layers)]


def sweep(blocks, materials, near, far, table):
    half = len(blocks)
    layers, rows, columns = blocks[0].shape[1:]
    f32 = jnp.float32
    cells = half * layers * rows * columns
    outs = pl.pallas_call(
        functools.partial(sweep_kernel, half),
        out_shape=[jax.ShapeDtypeStruct((layers, rows, columns), f32)] * half
        + [jax.ShapeDtypeStruct((4, rows, columns), f32)],
        in_specs=[VMEM] * (2 * half + 3),
        out_specs=[VMEM] * (half + 1),
        scratch_shapes=[
            pltpu.VMEM((2, (half + 2) * layers, rows, columns), f32),
            pltpu.VMEM((half * layers, rows, columns), jnp.int32),
            pltpu.VMEM((half * layers, rows, columns), f32),
        ],
        cost_estimate=pl.CostEstimate(flops=200 * cells, bytes_accessed=16 * cells, transcendentals=6 * cells),
        name="sweep",
    )(*blocks, *materials, near, far, table)
    return outs[:half], outs[half]


def over(nearer, farther):
    through = 1.0 - nearer[3:4]
    return jnp.concatenate([nearer[:3] + through * farther[:3], nearer[3:4] + through * farther[3:4]], axis=0)


def per_device(fluid_state, material, table_colour, table_extinction):
    slabs = lax.axis_size("slab")
    members = lax.axis_size("swap")
    half = members // 2
    member = lax.axis_index("swap")
    slab = lax.axis_index("slab")
    chip, upper = member // 2, member % 2
    _, layers, height, width = fluid_state.shape
    rows = height // half
    forward = routes(members)
    backward = [[(b, a) for a, b in pairs] for pairs in forward]

    scale = DEPTH_SCALE / (layers * slabs * members)
    table = jnp.concatenate([table_extinction[None] * scale, table_colour], axis=0)
    table = jnp.pad(table, ((0, 0), (0, LANES - table.shape[1])))
    table = jnp.broadcast_to(table[:, None, :], (4, 8, LANES))

    place = member % half
    blocks, materials = [], []
    for r in range(half):
        chunk = lax.dynamic_slice_in_dim(fluid_state, (place ^ r) * rows, rows, axis=2)
        blocks.append(lax.ppermute(chunk, "swap", forward[r]))
    for r in range(half):
        chunk = lax.dynamic_slice_in_dim(material, (place ^ r) * rows, rows, axis=1)
        materials.append(lax.ppermute(chunk, "swap", forward[r]))

    first = pick(blocks, chip)
    final = pick(blocks, chip ^ (half - 1))
    outer = jnp.where(upper == 1, final, first)
    inner = jnp.where(upper == 1, first, final)
    ring = []
    for z in range(slabs):
        for w in range(members):
            to = ((z + 1) % slabs, w - 1) if w % 2 else ((z - 1) % slabs, w + 1)
            ring.append((z * members + w, to[0] * members + to[1]))
    far = lax.ppermute(outer, ("slab", "swap"), ring)
    near = lax.ppermute(inner, "swap", [(w, w ^ 1) for w in range(members)])

    returned, image = sweep(blocks, materials, near, far, table)

    image = image.reshape(4, 2, rows // 2, width)
    kept = lax.dynamic_index_in_dim(image, upper, 1, keepdims=False)
    given = lax.dynamic_index_in_dim(image, 1 - upper, 1, keepdims=False)
    got = lax.ppermute(given, "swap", [(w, w ^ 1) for w in range(members)])
    tile = over(jnp.where(upper == 1, got, kept), jnp.where(upper == 1, kept, got))
    pieces = [tile]
    for away in range(1, slabs):
        pieces.append(lax.ppermute(tile, "slab", [(z, z ^ away) for z in range(slabs)]))
    chunks = [lax.ppermute(returned[r], "swap", backward[r]) for r in range(half)]
    ordered = [pick(pieces, slab ^ z) for z in range(slabs)]
    rendered = functools.reduce(over, ordered).reshape(4, height * width // members)
    density = jnp.concatenate([pick(chunks, place ^ j) for j in range(half)], axis=1)
    return density, rendered


def solution(mesh):
    return jax.shard_map(
        per_device,
        mesh=mesh,
        in_specs=(P(None, ("slab", "swap"), None, None), P(("slab", "swap"), None, None), P(), P()),
        out_specs=(P(("slab", "swap"), None, None), P(None, "swap")),
        check_vma=False,
    )
```

```python
import functools

import jax
import jax.numpy as jnp
from jax import lax
from jax.experimental import pallas as pl
from jax.experimental.pallas import tpu as pltpu
from jax.sharding import PartitionSpec as P

COURANT = 0.4
DEPTH_SCALE = 2.5
LANES = 128
F32 = jnp.float32
VMEM = pl.BlockSpec(memory_space=pltpu.VMEM)


def swap_pairs(members, mask):
    return [(w, w ^ mask) for w in range(members)]


def pick(arrays, index):
    out = arrays[0]
    for number in range(1, len(arrays)):
        out = jnp.where(index == number, arrays[number], out)
    return out


def advance(state, stage, density, momentum, emit):
    if stage == 4:
        emit(density)
        return
    last = stage == 3
    velocity = momentum / density
    speed = jnp.abs(velocity) + 1.0
    pressure = None if last else momentum * velocity + density
    held = state[stage]
    if held is None:
        state[stage] = (density, momentum, speed, pressure, None, None)
        return
    density0, momentum0, speed0, pressure0, mass0, force0 = held
    face = jnp.maximum(speed0, speed)
    mass = (momentum0 + momentum) - face * (density - density0)
    force = None if last else (pressure0 + pressure) - face * (momentum - momentum0)
    state[stage] = (density, momentum, speed, pressure, mass, force)
    if mass0 is None:
        return
    density1 = density0 - (0.5 * COURANT) * (mass - mass0)
    momentum1 = None if last else momentum0 - (0.5 * COURANT) * (force - force0)
    advance(state, stage + 1, density1, momentum1, emit)


def sweep_tiles(rows, columns, layers, count, backwards, load, dense_at, dense, kind_at, kind, table, finish):
    tall = min(8, rows)
    across = columns // LANES

    def tile(number, carry):
        row = pl.ds(pl.multiple_of(number // across * tall, tall), tall)
        column = pl.ds(pl.multiple_of(number % across * LANES, LANES), LANES)

        def block(state, light, position):
            for layer in range(layers):
                at = position * layers + layer

                def emit(density):
                    own = at - 2 * layers
                    dense[dense_at(own), row, column] = density
                    which = kind[kind_at(own), row, column]
                    factor, red, green, blue = (
                        jnp.take_along_axis(table[n, :tall, :], which, axis=1) for n in range(4)
                    )
                    through = jnp.exp(-(factor * density))
                    hidden = 1.0 - through
                    weight = jnp.where(backwards, hidden, hidden * light[0])
                    keep = jnp.where(backwards, through, 1.0)
                    light[0] = light[0] * through
                    light[1] = light[1] * keep + weight * red
                    light[2] = light[2] * keep + weight * green
                    light[3] = light[3] * keep + weight * blue

                advance(state, 0, *load(at, row, column), emit)

        state = [None] * 4
        zero = jnp.zeros((tall, LANES), F32)
        light = [zero + 1.0, zero, zero, zero]
        block(state, light, 0)
        block(state, light, 1)
        if count <= 5:
            for position in range(2, count):
                block(state, light, position)
        else:

            def step(position, carry):
                state, light = [list(part) for part in carry]
                block(state, light, position)
                return state, light

            state, light = lax.fori_loop(2, count, step, (state, light))
        finish(light, row, column)
        return carry

    lax.fori_loop(0, rows // tall * across, tile, 0)


def inner_kernel(chips, *refs):
    own, own_kind = refs[:chips], refs[chips : 2 * chips]
    other, other_kind, table, dense, image, edge, edge_kind, fluid, kind = refs[2 * chips :]
    member = lax.axis_index("swap")
    chip, upper = member // 2, member % 2
    half = chips // 2
    _, layers, rows, columns = own[0].shape
    shift = upper
    for d in range(chips):
        k = chip ^ d

        @pl.when(k // half == upper)
        def _():
            at = 2 * (k - upper * half) + upper
            fluid[:, pl.ds((at + shift) * layers, layers)] = own[d][...]
            kind[pl.ds(at * layers, layers)] = own_kind[d][...]

        @pl.when(k == jnp.where(upper == 1, half - 1, half))
        def _():
            at = jnp.where(upper == 1, 0, chips)
            fluid[:, pl.ds(at * layers, layers)] = own[d][...]

    for i in range(half):
        at = 2 * i + 1 - upper
        fluid[:, pl.ds((at + shift) * layers, layers)] = other[i]
        kind[pl.ds(at * layers, layers)] = other_kind[i]

    total = (chips + 1) * layers
    sign = jnp.where(upper == 1, 1.0, -1.0)

    def load(at, row, column):
        at = jnp.where(upper == 1, at, total - 1 - at)
        return fluid[0, at, row, column], sign * fluid[1, at, row, column]

    def place(own):
        return jnp.where(upper == 1, own, chips * layers - 1 - own)

    def finish(light, row, column):
        for n in range(4):
            image[n, row, column] = light[n]

    sweep_tiles(rows, columns, layers, chips + 1, upper == 0, load, place, dense, place, kind, table, finish)
    start = jnp.where(upper == 1, chips - 1, 0) * layers
    edge[...] = fluid[:, pl.ds(start, 2 * layers)]
    start = jnp.where(upper == 1, chips - 1, 0) * layers
    edge_kind[...] = kind[pl.ds(start, layers)]


def outer_kernel(chips, far, edge, edge_kind, table, dense, image, keep, give, tile, last, drawn):
    upper = lax.axis_index("swap") % 2
    half = chips // 2
    _, layers, rows, columns = far.shape
    sign = jnp.where(upper == 1, -1.0, 1.0)

    def load(at, row, column):
        source, base, size = (far, at, layers) if at < layers else (edge, at - layers, 2 * layers)
        base = jnp.where(upper == 1, size - 1 - base, base)
        return source[0, base, row, column], sign * source[1, base, row, column]

    def place(own):
        return jnp.where(upper == 1, layers - 1 - own, own)

    def finish(light, row, column):
        inner = [image[n, row, column] for n in range(4)]
        front = [jnp.where(upper == 1, a, b) for a, b in zip(inner, light)]
        back = [jnp.where(upper == 1, b, a) for a, b in zip(inner, light)]
        drawn[3, row, column] = front[0] * back[0]
        for n in range(1, 4):
            drawn[n - 1, row, column] = front[n] + front[0] * back[n]

    sweep_tiles(rows, columns, layers, 3, upper == 1, load, place, last, place, edge_kind, table, finish)
    for i in range(half):
        keep[i] = dense[pl.ds((2 * i + upper) * layers, layers)]
        give[pl.ds(i * layers, layers)] = dense[pl.ds((2 * i + 1 - upper) * layers, layers)]

    @pl.when(upper == 0)
    def _():
        keep[0] = last[...]

    @pl.when(upper == 1)
    def _():
        keep[half - 1] = last[...]

    short = rows // 2
    for n in range(4):
        low, high = drawn[n, :short], drawn[n, short:]
        tile[n] = jnp.where(upper == 1, high, low)
        given = jnp.where(upper == 1, low, high)
        give[half * layers + n // 2, (n % 2) * short : (n % 2 + 1) * short] = given


def cost(cells):
    return pl.CostEstimate(flops=300 * cells, bytes_accessed=16 * cells, transcendentals=6 * cells)


def sweep_inner(own, own_kind, other, other_kind, table):
    chips = len(own)
    _, layers, rows, columns = own[0].shape
    shape = lambda *dims, dtype=F32: jax.ShapeDtypeStruct((*dims, rows, columns), dtype)
    return pl.pallas_call(
        functools.partial(inner_kernel, chips),
        out_shape=[
            shape(chips * layers),
            shape(4),
            shape(2, 2 * layers),
            shape(layers, dtype=jnp.int32),
        ],
        in_specs=[VMEM] * (2 * chips + 3),
        out_specs=[VMEM] * 4,
        scratch_shapes=[
            pltpu.VMEM((2, (chips + 1) * layers, rows, columns), F32),
            pltpu.VMEM((chips * layers, rows, columns), jnp.int32),
        ],
        cost_estimate=cost(chips * layers * rows * columns),
        name="sweep_inner",
    )(*own, *own_kind, other, other_kind, table)


def sweep_outer(far, edge, edge_kind, table, dense, image):
    layers, rows, columns = edge_kind.shape
    half = dense.shape[0] // layers // 2
    shape = lambda *dims: jax.ShapeDtypeStruct(dims, F32)
    return pl.pallas_call(
        functools.partial(outer_kernel, 2 * half),
        out_shape=[
            shape(half, layers, rows, columns),
            shape(half * layers + 2, rows, columns),
            shape(4, rows // 2, columns),
        ],
        in_specs=[VMEM] * 6,
        out_specs=[VMEM] * 3,
        scratch_shapes=[
            pltpu.VMEM((layers, rows, columns), F32),
            pltpu.VMEM((4, rows, columns), F32),
        ],
        cost_estimate=cost(layers * rows * columns),
        name="sweep_outer",
    )(far, edge, edge_kind, table, dense, image)


def over(nearer, farther):
    return jnp.concatenate([nearer[:3] + nearer[3:4] * farther[:3], nearer[3:4] * farther[3:4]], axis=0)


def per_device(fluid_state, material, table_colour, table_extinction):
    slabs = lax.axis_size("slab")
    members = lax.axis_size("swap")
    chips = members // 2
    half = chips // 2
    member = lax.axis_index("swap")
    slab = lax.axis_index("slab")
    chip, upper = member // 2, member % 2
    _, layers, height, width = fluid_state.shape
    rows = height // chips

    def to_chip(block, d):
        return lax.ppermute(block, "swap", swap_pairs(members, 2 * d)) if d else block

    def to_core(block):
        return lax.ppermute(block, "swap", swap_pairs(members, 1))

    scale = DEPTH_SCALE / (layers * slabs * members)
    table = jnp.concatenate([table_extinction[None] * scale, table_colour], axis=0)
    table = jnp.pad(table, ((0, 0), (0, LANES - table.shape[1])))
    table = jnp.broadcast_to(table[:, None, :], (4, 8, LANES))

    own = [
        to_chip(lax.dynamic_slice_in_dim(fluid_state, (chip ^ d) * rows, rows, axis=2), d) for d in range(chips)
    ]
    own_kind = [
        to_chip(lax.dynamic_slice_in_dim(material, (chip ^ d) * rows, rows, axis=1), d) for d in range(chips)
    ]

    def others(blocks):
        return jnp.stack([pick(blocks, chip ^ ((1 - upper) * half + i)) for i in range(half)])

    other = to_core(others(own))
    ring = []
    for z in range(slabs):
        for w in range(members):
            to = ((z + 1) % slabs, w - 1) if w % 2 else ((z - 1) % slabs, w + 1)
            ring.append((z * members + w, to[0] * members + to[1]))
    far = lax.ppermute(pick(own, chip ^ (upper * (chips - 1))), ("slab", "swap"), ring)
    other_kind = to_core(others(own_kind))

    dense, image, edge, edge_kind = sweep_inner(own, own_kind, other, other_kind, table)
    keep, give, tile = sweep_outer(far, edge, edge_kind, table, dense, image)
    got = to_core(give)

    partner = got[half * layers :].reshape(4, rows // 2, width)
    tile = over(jnp.where(upper == 1, partner, tile), jnp.where(upper == 1, tile, partner))
    pieces = [tile]
    for away in range(1, slabs):
        pieces.append(lax.ppermute(tile, "slab", swap_pairs(slabs, away)))
    ordered = [pick(pieces, slab ^ z) for z in range(slabs)]
    rendered = functools.reduce(over, ordered)
    rendered = jnp.concatenate([rendered[:3], 1.0 - rendered[3:4]], axis=0).reshape(4, height * width // members)

    kept = [keep[i] for i in range(half)]
    gotten = [got[i * layers : (i + 1) * layers] for i in range(half)]
    chunks = []
    for d in range(chips):
        k = chip ^ d
        block = jnp.where(k // half == upper, pick(kept, k % half), pick(gotten, k % half))
        chunks.append(to_chip(block, d))
    density = jnp.concatenate([pick(chunks, chip ^ j) for j in range(chips)], axis=1)
    return density, rendered


def solution(mesh):
    return jax.shard_map(
        per_device,
        mesh=mesh,
        in_specs=(P(None, ("slab", "swap"), None, None), P(("slab", "swap"), None, None), P(), P()),
        out_specs=(P(("slab", "swap"), None, None), P(None, "swap")),
        check_vma=False,
    )
```

```python
import functools

import jax
import jax.numpy as jnp
from jax import lax
from jax.experimental import pallas as pl
from jax.experimental.pallas import tpu as pltpu
from jax.sharding import PartitionSpec as P

COURANT = 0.4
DEPTH_SCALE = 2.5
LANES = 128
F32 = jnp.float32
GRANT = 12 << 20
VMEM = pl.BlockSpec(memory_space=pltpu.VMEM)


def swap_pairs(members, mask):
    return [(w, w ^ mask) for w in range(members)]


def pick(arrays, index):
    out = arrays[0]
    for number in range(1, len(arrays)):
        out = jnp.where(index == number, arrays[number], out)
    return out


def advance(state, stage, density, momentum, emit):
    if stage == 4:
        emit(density)
        return
    last = stage == 3
    velocity = momentum / density
    speed = jnp.abs(velocity) + 1.0
    pressure = None if last else momentum * velocity + density
    held = state[stage]
    if held is None:
        state[stage] = (density, momentum, speed, pressure, None, None)
        return
    density0, momentum0, speed0, pressure0, mass0, force0 = held
    face = jnp.maximum(speed0, speed)
    mass = (momentum0 + momentum) - face * (density - density0)
    force = None if last else (pressure0 + pressure) - face * (momentum - momentum0)
    state[stage] = (density, momentum, speed, pressure, mass, force)
    if mass0 is None:
        return
    density1 = density0 - (0.5 * COURANT) * (mass - mass0)
    momentum1 = None if last else momentum0 - (0.5 * COURANT) * (force - force0)
    advance(state, stage + 1, density1, momentum1, emit)


def sweep_tiles(rows, columns, layers, count, backwards, load, dense_at, dense, kind_at, kind, table, finish):
    tall = min(8, rows)
    across = columns // LANES

    def tile(number, carry):
        row = pl.ds(pl.multiple_of(number // across * tall, tall), tall)
        column = pl.ds(pl.multiple_of(number % across * LANES, LANES), LANES)

        def block(state, light, position):
            for layer in range(layers):
                at = position * layers + layer

                def emit(density):
                    own = at - 2 * layers
                    dense[dense_at(own), row, column] = density
                    which = kind[kind_at(own), row, column]
                    factor, red, green, blue = (
                        jnp.take_along_axis(table[n, :tall, :], which, axis=1) for n in range(4)
                    )
                    through = jnp.exp(-(factor * density))
                    hidden = 1.0 - through
                    weight = jnp.where(backwards, hidden, hidden * light[0])
                    keep = jnp.where(backwards, through, 1.0)
                    light[0] = light[0] * through
                    light[1] = light[1] * keep + weight * red
                    light[2] = light[2] * keep + weight * green
                    light[3] = light[3] * keep + weight * blue

                advance(state, 0, *load(at, row, column), emit)

        state = [None] * 4
        zero = jnp.zeros((tall, LANES), F32)
        light = [zero + 1.0, zero, zero, zero]
        block(state, light, 0)
        block(state, light, 1)
        if count <= 5:
            for position in range(2, count):
                block(state, light, position)
        else:

            def step(position, carry):
                state, light = [list(part) for part in carry]
                block(state, light, position)
                return state, light

            state, light = lax.fori_loop(2, count, step, (state, light))
        finish(light, row, column)
        return carry

    lax.fori_loop(0, rows // tall * across, tile, 0)


def inner_kernel(chips, *refs):
    own, own_kind = refs[:chips], refs[chips : 2 * chips]
    other, other_kind, table, dense, image, edge, edge_kind, fluid, kind = refs[2 * chips :]
    member = lax.axis_index("swap")
    chip, upper = member // 2, member % 2
    half = chips // 2
    _, layers, rows, columns = own[0].shape
    shift = upper
    for d in range(chips):
        k = chip ^ d

        @pl.when(k // half == upper)
        def _():
            at = 2 * (k - upper * half) + upper
            fluid[:, pl.ds((at + shift) * layers, layers)] = own[d][...]
            kind[pl.ds(at * layers, layers)] = own_kind[d][...]

        @pl.when(k == jnp.where(upper == 1, half - 1, half))
        def _():
            at = jnp.where(upper == 1, 0, chips)
            fluid[:, pl.ds(at * layers, layers)] = own[d][...]

    for i in range(half):
        at = 2 * i + 1 - upper
        fluid[:, pl.ds((at + shift) * layers, layers)] = other[i]
        kind[pl.ds(at * layers, layers)] = other_kind[i]

    total = (chips + 1) * layers
    sign = jnp.where(upper == 1, 1.0, -1.0)

    def load(at, row, column):
        at = jnp.where(upper == 1, at, total - 1 - at)
        return fluid[0, at, row, column], sign * fluid[1, at, row, column]

    def place(own):
        return jnp.where(upper == 1, own, chips * layers - 1 - own)

    def finish(light, row, column):
        for n in range(4):
            image[n, row, column] = light[n]

    sweep_tiles(rows, columns, layers, chips + 1, upper == 0, load, place, dense, place, kind, table, finish)
    start = jnp.where(upper == 1, chips - 1, 0) * layers
    edge[...] = fluid[:, pl.ds(start, 2 * layers)]
    start = jnp.where(upper == 1, chips - 1, 0) * layers
    edge_kind[...] = kind[pl.ds(start, layers)]


def outer_kernel(chips, far, edge, edge_kind, table, dense, image, keep, give, tile, last, drawn):
    upper = lax.axis_index("swap") % 2
    half = chips // 2
    _, layers, rows, columns = far.shape
    sign = jnp.where(upper == 1, -1.0, 1.0)

    def load(at, row, column):
        source, base, size = (far, at, layers) if at < layers else (edge, at - layers, 2 * layers)
        base = jnp.where(upper == 1, size - 1 - base, base)
        return source[0, base, row, column], sign * source[1, base, row, column]

    def place(own):
        return jnp.where(upper == 1, layers - 1 - own, own)

    def finish(light, row, column):
        inner = [image[n, row, column] for n in range(4)]
        front = [jnp.where(upper == 1, a, b) for a, b in zip(inner, light)]
        back = [jnp.where(upper == 1, b, a) for a, b in zip(inner, light)]
        drawn[3, row, column] = front[0] * back[0]
        for n in range(1, 4):
            drawn[n - 1, row, column] = front[n] + front[0] * back[n]

    sweep_tiles(rows, columns, layers, 3, upper == 1, load, place, last, place, edge_kind, table, finish)
    for i in range(half):
        keep[i] = dense[pl.ds((2 * i + upper) * layers, layers)]
        give[pl.ds(i * layers, layers)] = dense[pl.ds((2 * i + 1 - upper) * layers, layers)]

    @pl.when(upper == 0)
    def _():
        keep[0] = last[...]

    @pl.when(upper == 1)
    def _():
        keep[half - 1] = last[...]

    short = rows // 2
    for n in range(4):
        low, high = drawn[n, :short], drawn[n, short:]
        tile[n] = jnp.where(upper == 1, high, low)
        given = jnp.where(upper == 1, low, high)
        give[half * layers + n // 2, (n % 2) * short : (n % 2 + 1) * short] = given


def route_kernel(chips, with_far, *refs):
    own, given = refs[:chips], refs[chips]
    member = lax.axis_index("swap")
    chip, upper = member // 2, member % 2
    half = chips // 2
    for d in range(chips):
        k = chip ^ d

        @pl.when(k // half != upper)
        def _():
            given[k - (1 - upper) * half] = own[d][...]

        if with_far:

            @pl.when(k == upper * (chips - 1))
            def _():
                refs[chips + 1][...] = own[d][...]


def route(blocks, with_far):
    chips = len(blocks)
    shape, dtype = blocks[0].shape, blocks[0].dtype
    shapes = [jax.ShapeDtypeStruct((chips // 2, *shape), dtype)] + [jax.ShapeDtypeStruct(shape, dtype)] * with_far
    return pl.pallas_call(
        functools.partial(route_kernel, chips, with_far),
        out_shape=shapes,
        in_specs=[VMEM] * chips,
        out_specs=[VMEM] * len(shapes),
        compiler_params=pltpu.CompilerParams(vmem_limit_bytes=GRANT),
        cost_estimate=pl.CostEstimate(flops=1000, bytes_accessed=1 << 20, transcendentals=0),
        name="route",
    )(*blocks)


def cost(cells):
    return pl.CostEstimate(flops=300 * cells, bytes_accessed=16 * cells, transcendentals=6 * cells)


def sweep_inner(own, own_kind, other, other_kind, table):
    chips = len(own)
    _, layers, rows, columns = own[0].shape
    shape = lambda *dims, dtype=F32: jax.ShapeDtypeStruct((*dims, rows, columns), dtype)
    return pl.pallas_call(
        functools.partial(inner_kernel, chips),
        out_shape=[
            shape(chips * layers),
            shape(4),
            shape(2, 2 * layers),
            shape(layers, dtype=jnp.int32),
        ],
        in_specs=[VMEM] * (2 * chips + 3),
        out_specs=[VMEM] * 4,
        scratch_shapes=[
            pltpu.VMEM((2, (chips + 1) * layers, rows, columns), F32),
            pltpu.VMEM((chips * layers, rows, columns), jnp.int32),
        ],
        cost_estimate=cost(chips * layers * rows * columns),
        compiler_params=pltpu.CompilerParams(vmem_limit_bytes=GRANT),
        name="sweep_inner",
    )(*own, *own_kind, other, other_kind, table)


def sweep_outer(far, edge, edge_kind, table, dense, image):
    layers, rows, columns = edge_kind.shape
    half = dense.shape[0] // layers // 2
    shape = lambda *dims: jax.ShapeDtypeStruct(dims, F32)
    return pl.pallas_call(
        functools.partial(outer_kernel, 2 * half),
        out_shape=[
            shape(half, layers, rows, columns),
            shape(half * layers + 2, rows, columns),
            shape(4, rows // 2, columns),
        ],
        in_specs=[VMEM] * 6,
        out_specs=[VMEM] * 3,
        scratch_shapes=[
            pltpu.VMEM((layers, rows, columns), F32),
            pltpu.VMEM((4, rows, columns), F32),
        ],
        cost_estimate=cost(layers * rows * columns),
        compiler_params=pltpu.CompilerParams(vmem_limit_bytes=GRANT),
        name="sweep_outer",
    )(far, edge, edge_kind, table, dense, image)


def over(nearer, farther):
    return jnp.concatenate([nearer[:3] + nearer[3:4] * farther[:3], nearer[3:4] * farther[3:4]], axis=0)


def per_device(fluid_state, material, table_colour, table_extinction):
    slabs = lax.axis_size("slab")
    members = lax.axis_size("swap")
    chips = members // 2
    half = chips // 2
    member = lax.axis_index("swap")
    slab = lax.axis_index("slab")
    chip, upper = member // 2, member % 2
    _, layers, height, width = fluid_state.shape
    rows = height // chips

    def to_chip(block, d):
        if d == 0:
            return block
        return lax.ppermute(block, "swap", swap_pairs(members, 2 * d))

    def to_core(block):
        return lax.ppermute(block, "swap", swap_pairs(members, 1))

    scale = DEPTH_SCALE / (layers * slabs * members)
    table = jnp.concatenate([table_extinction[None] * scale, table_colour], axis=0)
    table = jnp.pad(table, ((0, 0), (0, LANES - table.shape[1])))
    table = jnp.broadcast_to(table[:, None, :], (4, 8, LANES))

    sent = [lax.dynamic_slice_in_dim(fluid_state, (chip ^ d) * rows, rows, axis=2) for d in range(chips)]
    own = [to_chip(sent[d], d) for d in range(chips)]
    own_kind = [to_chip(lax.dynamic_slice_in_dim(material, (chip ^ d) * rows, rows, axis=1), d) for d in range(chips)]
    other, outer = route(own, True)
    *own_kind, table, _ = lax.optimization_barrier((*own_kind, table, outer))
    other = to_core(other)
    ring = []
    for z in range(slabs):
        for w in range(members):
            to = ((z + 1) % slabs, w - 1) if w % 2 else ((z - 1) % slabs, w + 1)
            ring.append((z * members + w, to[0] * members + to[1]))
    far = lax.ppermute(outer, ("slab", "swap"), ring)
    other_kind = to_core(route(own_kind, False)[0])

    dense, image, edge, edge_kind = sweep_inner(own, own_kind, other, other_kind, table)
    keep, give, tile = sweep_outer(far, edge, edge_kind, table, dense, image)
    got = to_core(give)

    kept = [keep[i] for i in range(half)]
    gotten = [got[i * layers : (i + 1) * layers] for i in range(half)]
    chunks = []
    for d in range(chips):
        k = chip ^ d
        block = jnp.where(k // half == upper, pick(kept, k % half), pick(gotten, k % half))
        chunks.append(to_chip(block, d))
    density = jnp.concatenate([pick(chunks, chip ^ j) for j in range(chips)], axis=1)

    partner = got[half * layers :].reshape(4, rows // 2, width)
    tile = over(jnp.where(upper == 1, partner, tile), jnp.where(upper == 1, tile, partner))
    pieces = [tile]
    for away in range(1, slabs):
        pieces.append(lax.ppermute(tile, "slab", swap_pairs(slabs, away)))
    ordered = [pick(pieces, slab ^ z) for z in range(slabs)]
    rendered = functools.reduce(over, ordered)
    rendered = jnp.concatenate([rendered[:3], 1.0 - rendered[3:4]], axis=0).reshape(4, height * width // members)
    return density, rendered


def solution(mesh):
    return jax.shard_map(
        per_device,
        mesh=mesh,
        in_specs=(P(None, ("slab", "swap"), None, None), P(("slab", "swap"), None, None), P(), P()),
        out_specs=(P(("slab", "swap"), None, None), P(None, "swap")),
        check_vma=False,
    )
```

```python
import functools

import jax
import jax.numpy as jnp
from jax import lax
from jax.experimental import pallas as pl
from jax.experimental.pallas import tpu as pltpu
from jax.sharding import PartitionSpec as P

COURANT = 0.4
DEPTH_SCALE = 2.5
LANES = 128
F32 = jnp.float32
GRANT = 12 << 20
VMEM = pl.BlockSpec(memory_space=pltpu.VMEM)


def swap_pairs(members, mask):
    return [(w, w ^ mask) for w in range(members)]


def pick(arrays, index):
    out = arrays[0]
    for number in range(1, len(arrays)):
        out = jnp.where(index == number, arrays[number], out)
    return out


def advance(state, stage, density, momentum, emit):
    if stage == 4:
        emit(density)
        return
    last = stage == 3
    velocity = momentum / density
    speed = jnp.abs(velocity) + 1.0
    pressure = None if last else momentum * velocity + density
    held = state[stage]
    if held is None:
        state[stage] = (density, momentum, speed, pressure, None, None)
        return
    density0, momentum0, speed0, pressure0, mass0, force0 = held
    face = jnp.maximum(speed0, speed)
    mass = (momentum0 + momentum) - face * (density - density0)
    force = None if last else (pressure0 + pressure) - face * (momentum - momentum0)
    state[stage] = (density, momentum, speed, pressure, mass, force)
    if mass0 is None:
        return
    density1 = density0 - (0.5 * COURANT) * (mass - mass0)
    momentum1 = None if last else momentum0 - (0.5 * COURANT) * (force - force0)
    advance(state, stage + 1, density1, momentum1, emit)


def sweep_tiles(rows, columns, layers, count, load, place, dense):
    tall = min(8, rows)
    across = columns // LANES

    def tile(number, carry):
        row = pl.ds(pl.multiple_of(number // across * tall, tall), tall)
        column = pl.ds(pl.multiple_of(number % across * LANES, LANES), LANES)

        def block(state, position):
            for layer in range(layers):
                at = position * layers + layer

                def emit(density):
                    dense[place(at - 2 * layers), row, column] = density

                advance(state, 0, *load(at, row, column), emit)

        state = [None] * 4
        block(state, 0)
        block(state, 1)
        if count <= 5:
            for position in range(2, count):
                block(state, position)
        else:

            def step(position, state):
                state = list(state)
                block(state, position)
                return state

            lax.fori_loop(2, count, step, state)
        return carry

    lax.fori_loop(0, rows // tall * across, tile, 0)


def inner_kernel(chips, *refs):
    own, (other, dense, edge, fluid) = refs[:chips], refs[chips:]
    member = lax.axis_index("swap")
    chip, upper = member // 2, member % 2
    half = chips // 2
    _, layers, rows, columns = own[0].shape
    for d in range(chips):
        k = chip ^ d

        @pl.when(k // half == upper)
        def _():
            at = 2 * (k - upper * half) + 2 * upper
            fluid[:, pl.ds(at * layers, layers)] = own[d][...]

        @pl.when(k == jnp.where(upper == 1, half - 1, half))
        def _():
            at = jnp.where(upper == 1, 0, chips)
            fluid[:, pl.ds(at * layers, layers)] = own[d][...]

    for i in range(half):
        fluid[:, pl.ds((2 * i + 1) * layers, layers)] = other[i]

    total = (chips + 1) * layers
    sign = jnp.where(upper == 1, 1.0, -1.0)

    def load(at, row, column):
        at = jnp.where(upper == 1, at, total - 1 - at)
        return fluid[0, at, row, column], sign * fluid[1, at, row, column]

    def place(own):
        return jnp.where(upper == 1, own, chips * layers - 1 - own)

    sweep_tiles(rows, columns, layers, chips + 1, load, place, dense)
    edge[...] = fluid[:, pl.ds(jnp.where(upper == 1, chips - 1, 0) * layers, 2 * layers)]


def outer_kernel(chips, far, edge, dense, keep, give, last):
    upper = lax.axis_index("swap") % 2
    half = chips // 2
    _, layers, rows, columns = far.shape
    sign = jnp.where(upper == 1, -1.0, 1.0)

    def load(at, row, column):
        source, base, size = (far, at, layers) if at < layers else (edge, at - layers, 2 * layers)
        base = jnp.where(upper == 1, size - 1 - base, base)
        return source[0, base, row, column], sign * source[1, base, row, column]

    def place(own):
        return jnp.where(upper == 1, layers - 1 - own, own)

    sweep_tiles(rows, columns, layers, 3, load, place, last)
    for i in range(half):
        keep[i] = dense[pl.ds((2 * i + upper) * layers, layers)]
        give[i] = dense[pl.ds((2 * i + 1 - upper) * layers, layers)]
    keep[jnp.where(upper == 1, half - 1, 0)] = last[...]


def render_kernel(chips, *refs):
    kinds, (table, keep, given, tile, sent, dense, kind) = refs[:chips], refs[chips:]
    member = lax.axis_index("swap")
    chip, upper = member // 2, member % 2
    half, layers, rows, columns = keep.shape
    for d in range(chips):
        k = chip ^ d

        @pl.when(k // half == upper)
        def _():
            kind[pl.ds(2 * (k - upper * half) * layers, 2 * layers)] = kinds[d][...].reshape(2 * layers, rows, columns)

    for i in range(half):
        dense[pl.ds((2 * i + upper) * layers, layers)] = keep[i]
        dense[pl.ds((2 * i + 1 - upper) * layers, layers)] = given[i]

    tall = min(8, rows // 2)
    across = columns // LANES
    tables = [table[n, :tall, :] for n in range(4)]

    def shade(at, light, row, column):
        which = kind[at, row, column]
        factor, *colours = (jnp.take_along_axis(values, which, axis=1) for values in tables)
        through = jnp.exp(-(factor * dense[at, row, column]))
        weight = light[0] * (1.0 - through)
        return (light[0] * through, *(sum_ + weight * colour for sum_, colour in zip(light[1:], colours)))

    depth = chips * layers
    half_rows = rows // 2

    def strip(number, carry):
        column = pl.ds(pl.multiple_of(number * LANES, LANES), LANES)
        for row in range(0, rows, tall):
            zero = jnp.zeros((tall, LANES), F32)
            light = (zero + 1.0, zero, zero, zero)
            where = pl.ds(row, tall)
            if depth <= 16:
                for at in range(depth):
                    light = shade(at, light, where, column)
            else:
                light = lax.fori_loop(0, depth, lambda at, light: shade(at, light, where, column), light)
            base = row % half_rows
            for n, value in enumerate((*light[1:], light[0])):

                @pl.when(upper == row // half_rows)
                def _():
                    tile[n, base : base + tall, column] = value

                @pl.when(upper != row // half_rows)
                def _():
                    sent[n, base : base + tall, column] = value

        return carry

    lax.fori_loop(0, across, strip, 0)


def route_kernel(chips, *refs):
    own, (other, outer) = refs[:chips], refs[chips:]
    member = lax.axis_index("swap")
    chip, upper = member // 2, member % 2
    half = chips // 2
    for d in range(chips):
        k = chip ^ d

        @pl.when(k // half != upper)
        def _():
            other[k - (1 - upper) * half] = own[d][...]

        @pl.when(k == upper * (chips - 1))
        def _():
            outer[...] = own[d][...]


def call(kernel, operands, outs, scratch=(), cells=0):
    return pl.pallas_call(
        kernel,
        out_shape=[jax.ShapeDtypeStruct(shape, F32) for shape in outs],
        in_specs=[VMEM] * len(operands),
        out_specs=[VMEM] * len(outs),
        scratch_shapes=[pltpu.VMEM(shape, dtype) for shape, dtype in scratch],
        compiler_params=pltpu.CompilerParams(vmem_limit_bytes=GRANT),
        cost_estimate=pl.CostEstimate(flops=300 * cells, bytes_accessed=16 * cells, transcendentals=6 * cells),
    )(*operands)


def over(nearer, farther):
    return jnp.concatenate([nearer[:3] + nearer[3:4] * farther[:3], nearer[3:4] * farther[3:4]], axis=0)


def per_device(fluid_state, material, table_colour, table_extinction):
    slabs = lax.axis_size("slab")
    members = lax.axis_size("swap")
    chips = members // 2
    half = chips // 2
    member = lax.axis_index("swap")
    slab = lax.axis_index("slab")
    chip, upper = member // 2, member % 2
    _, layers, height, width = fluid_state.shape
    rows = height // chips

    def to_chip(block, d):
        if d == 0:
            return block
        return lax.ppermute(block, "swap", swap_pairs(members, 2 * d))

    def to_core(block):
        return lax.ppermute(block, "swap", swap_pairs(members, 1))

    scale = DEPTH_SCALE / (layers * slabs * members)
    table = jnp.concatenate([table_extinction[None] * scale, table_colour], axis=0)
    table = jnp.pad(table, ((0, 0), (0, LANES - table.shape[1])))
    table = jnp.broadcast_to(table[:, None, :], (4, 8, LANES))

    def cut(array, j, axis):
        return lax.dynamic_slice_in_dim(array, j * rows, rows, axis=axis)

    own = [to_chip(cut(fluid_state, chip ^ d, 2), d) for d in range(chips)]

    theirs = to_core(material)
    both = jnp.stack([jnp.where(upper == 1, theirs, material), jnp.where(upper == 1, material, theirs)])
    cuts = [cut(both, chip ^ d, 2) for d in range(chips)]
    senders = [w for w in range(members) if w % 2 == w // 2 // half]
    kinds = [cuts[0]]
    for d in range(1, chips):
        kinds.append(lax.ppermute(cuts[d], "swap", [(w, w ^ (2 * d)) for w in senders]))

    block = (layers, rows, width)
    cells = layers * rows * width
    other, outer = call(functools.partial(route_kernel, chips), own, [(half, 2, *block), (2, *block)])
    other = to_core(other)
    ring = []
    for z in range(slabs):
        for w in range(members):
            to = ((z + 1) % slabs, w - 1) if w % 2 else ((z - 1) % slabs, w + 1)
            ring.append((z * members + w, to[0] * members + to[1]))
    far = lax.ppermute(outer, ("slab", "swap"), ring)

    dense, edge = call(
        functools.partial(inner_kernel, chips),
        [*own, other],
        [(chips * layers, rows, width), (2, 2 * layers, rows, width)],
        [((2, (chips + 1) * layers, rows, width), F32)],
        chips * cells,
    )
    keep, give = call(
        functools.partial(outer_kernel, chips),
        [far, edge, dense],
        [(half, *block), (half, *block)],
        [(block, F32)],
        cells,
    )
    got = to_core(give)
    short = (4, rows // 2, width)
    tile, sent = call(
        functools.partial(render_kernel, chips),
        [*kinds, table, keep, give],
        [short, short],
        [((chips * layers, rows, width), F32), ((chips * layers, rows, width), jnp.int32)],
        chips * cells,
    )
    partner = to_core(sent)

    kept = [keep[i] for i in range(half)]
    gotten = [got[i] for i in range(half)]
    chunks = []
    for d in range(chips):
        k = chip ^ d
        back = jnp.where(k // half == upper, pick(kept, k % half), pick(gotten, k % half))
        chunks.append(to_chip(back, d))
    density = jnp.concatenate([pick(chunks, chip ^ j) for j in range(chips)], axis=1)

    tile = over(jnp.where(upper == 1, partner, tile), jnp.where(upper == 1, tile, partner))
    pieces = [tile]
    for away in range(1, slabs):
        pieces.append(lax.ppermute(tile, "slab", swap_pairs(slabs, away)))
    ordered = [pick(pieces, slab ^ z) for z in range(slabs)]
    rendered = functools.reduce(over, ordered)
    rendered = jnp.concatenate([rendered[:3], 1.0 - rendered[3:4]], axis=0).reshape(4, height * width // members)
    return density, rendered


def solution(mesh):
    return jax.shard_map(
        per_device,
        mesh=mesh,
        in_specs=(P(None, ("slab", "swap"), None, None), P(("slab", "swap"), None, None), P(), P()),
        out_specs=(P(("slab", "swap"), None, None), P(None, "swap")),
        check_vma=False,
    )
```

```python
import functools

import jax
import jax.numpy as jnp
from jax import lax
from jax.experimental import pallas as pl
from jax.experimental.pallas import tpu as pltpu
from jax.sharding import PartitionSpec as P

COURANT = 0.4
DEPTH_SCALE = 2.5
LANES = 128
F32 = jnp.float32
GRANT = 12 << 20
VMEM = pl.BlockSpec(memory_space=pltpu.VMEM)


def swap_pairs(members, mask):
    return [(w, w ^ mask) for w in range(members)]


def pick(arrays, index):
    out = arrays[0]
    for number in range(1, len(arrays)):
        out = jnp.where(index == number, arrays[number], out)
    return out


def advance(state, stage, density, momentum, emit):
    if stage == 4:
        emit(density)
        return
    last = stage == 3
    velocity = momentum / density
    speed = jnp.abs(velocity) + 1.0
    pressure = None if last else momentum * velocity + density
    held = state[stage]
    if held is None:
        state[stage] = (density, momentum, speed, pressure, None, None)
        return
    density0, momentum0, speed0, pressure0, mass0, force0 = held
    face = jnp.maximum(speed0, speed)
    mass = (momentum0 + momentum) - face * (density - density0)
    force = None if last else (pressure0 + pressure) - face * (momentum - momentum0)
    state[stage] = (density, momentum, speed, pressure, mass, force)
    if mass0 is None:
        return
    density1 = density0 - (0.5 * COURANT) * (mass - mass0)
    momentum1 = None if last else momentum0 - (0.5 * COURANT) * (force - force0)
    advance(state, stage + 1, density1, momentum1, emit)


def sweep_tiles(rows, columns, layers, count, backwards, load, dense_at, dense, kind_at, kind, table, finish):
    tall = min(8, rows)
    across = columns // LANES

    def tile(number, carry):
        row = pl.ds(pl.multiple_of(number // across * tall, tall), tall)
        column = pl.ds(pl.multiple_of(number % across * LANES, LANES), LANES)

        def block(state, light, position):
            for layer in range(layers):
                at = position * layers + layer

                def emit(density):
                    own = at - 2 * layers
                    dense[dense_at(own), row, column] = density
                    which = kind[kind_at(own), row, column]
                    factor, red, green, blue = (
                        jnp.take_along_axis(table[n, :tall, :], which, axis=1) for n in range(4)
                    )
                    through = jnp.exp(-(factor * density))
                    hidden = 1.0 - through
                    weight = jnp.where(backwards, hidden, hidden * light[0])
                    keep = jnp.where(backwards, through, 1.0)
                    light[0] = light[0] * through
                    light[1] = light[1] * keep + weight * red
                    light[2] = light[2] * keep + weight * green
                    light[3] = light[3] * keep + weight * blue

                advance(state, 0, *load(at, row, column), emit)

        state = [None] * 4
        zero = jnp.zeros((tall, LANES), F32)
        light = [zero + 1.0, zero, zero, zero]
        block(state, light, 0)
        block(state, light, 1)
        if count <= 5:
            for position in range(2, count):
                block(state, light, position)
        else:

            def step(position, carry):
                state, light = [list(part) for part in carry]
                block(state, light, position)
                return state, light

            state, light = lax.fori_loop(2, count, step, (state, light))
        finish(light, row, column)
        return carry

    lax.fori_loop(0, rows // tall * across, tile, 0)


def inner_kernel(chips, *refs):
    own, kinds = refs[:chips], refs[chips : 2 * chips]
    other, table, dense, image, edge, edge_kind, fluid, kind = refs[2 * chips :]
    member = lax.axis_index("swap")
    chip, upper = member // 2, member % 2
    half = chips // 2
    _, layers, rows, columns = own[0].shape
    for d in range(chips):
        k = chip ^ d

        @pl.when(k // half == upper)
        def _():
            at = 2 * (k - upper * half)
            fluid[:, pl.ds((at + 2 * upper) * layers, layers)] = own[d][...]
            kind[pl.ds(at * layers, 2 * layers)] = kinds[d][...].reshape(2 * layers, rows, columns)

        @pl.when(k == jnp.where(upper == 1, half - 1, half))
        def _():
            at = jnp.where(upper == 1, 0, chips)
            fluid[:, pl.ds(at * layers, layers)] = own[d][...]

    for i in range(half):
        fluid[:, pl.ds((2 * i + 1) * layers, layers)] = other[i]

    total = (chips + 1) * layers
    sign = jnp.where(upper == 1, 1.0, -1.0)

    def load(at, row, column):
        at = jnp.where(upper == 1, at, total - 1 - at)
        return fluid[0, at, row, column], sign * fluid[1, at, row, column]

    def place(own):
        return jnp.where(upper == 1, own, chips * layers - 1 - own)

    def finish(light, row, column):
        for n in range(4):
            image[n, row, column] = light[n]

    sweep_tiles(rows, columns, layers, chips + 1, upper == 0, load, place, dense, place, kind, table, finish)
    start = jnp.where(upper == 1, chips - 1, 0) * layers
    edge[...] = fluid[:, pl.ds(start, 2 * layers)]
    edge_kind[...] = kind[pl.ds(start, layers)]


def outer_kernel(chips, far, edge, edge_kind, table, dense, image, keep, give, tile, last, drawn):
    upper = lax.axis_index("swap") % 2
    half = chips // 2
    _, layers, rows, columns = far.shape
    sign = jnp.where(upper == 1, -1.0, 1.0)

    def load(at, row, column):
        source, base, size = (far, at, layers) if at < layers else (edge, at - layers, 2 * layers)
        base = jnp.where(upper == 1, size - 1 - base, base)
        return source[0, base, row, column], sign * source[1, base, row, column]

    def place(own):
        return jnp.where(upper == 1, layers - 1 - own, own)

    def finish(light, row, column):
        inner = [image[n, row, column] for n in range(4)]
        front = [jnp.where(upper == 1, a, b) for a, b in zip(inner, light)]
        back = [jnp.where(upper == 1, b, a) for a, b in zip(inner, light)]
        drawn[3, row, column] = front[0] * back[0]
        for n in range(1, 4):
            drawn[n - 1, row, column] = front[n] + front[0] * back[n]

    sweep_tiles(rows, columns, layers, 3, upper == 1, load, place, last, place, edge_kind, table, finish)
    for i in range(half):
        keep[i] = dense[pl.ds((2 * i + upper) * layers, layers)]
        give[pl.ds(i * layers, layers)] = dense[pl.ds((2 * i + 1 - upper) * layers, layers)]

    @pl.when(upper == 0)
    def _():
        keep[0] = last[...]

    @pl.when(upper == 1)
    def _():
        keep[half - 1] = last[...]

    short = rows // 2
    for n in range(4):
        low, high = drawn[n, :short], drawn[n, short:]
        tile[n] = jnp.where(upper == 1, high, low)
        given = jnp.where(upper == 1, low, high)
        give[half * layers + n // 2, (n % 2) * short : (n % 2 + 1) * short] = given


def route_kernel(chips, *refs):
    own, (other, outer) = refs[:chips], refs[chips:]
    member = lax.axis_index("swap")
    chip, upper = member // 2, member % 2
    half = chips // 2
    for d in range(chips):
        k = chip ^ d

        @pl.when(k // half != upper)
        def _():
            other[k - (1 - upper) * half] = own[d][...]

        @pl.when(k == upper * (chips - 1))
        def _():
            outer[...] = own[d][...]


def call(kernel, operands, outs, scratch=(), cells=0):
    return pl.pallas_call(
        kernel,
        out_shape=[jax.ShapeDtypeStruct(shape, dtype) for shape, dtype in outs],
        in_specs=[VMEM] * len(operands),
        out_specs=[VMEM] * len(outs),
        scratch_shapes=[pltpu.VMEM(shape, dtype) for shape, dtype in scratch],
        compiler_params=pltpu.CompilerParams(vmem_limit_bytes=GRANT),
        cost_estimate=pl.CostEstimate(flops=300 * cells, bytes_accessed=16 * cells, transcendentals=6 * cells),
    )(*operands)


def over(nearer, farther):
    return jnp.concatenate([nearer[:3] + nearer[3:4] * farther[:3], nearer[3:4] * farther[3:4]], axis=0)


def per_device(fluid_state, material, table_colour, table_extinction):
    slabs = lax.axis_size("slab")
    members = lax.axis_size("swap")
    chips = members // 2
    half = chips // 2
    member = lax.axis_index("swap")
    slab = lax.axis_index("slab")
    chip, upper = member // 2, member % 2
    _, layers, height, width = fluid_state.shape
    rows = height // chips

    def to_chip(block, d):
        if d == 0:
            return block
        return lax.ppermute(block, "swap", swap_pairs(members, 2 * d))

    def to_core(block):
        return lax.ppermute(block, "swap", swap_pairs(members, 1))

    scale = DEPTH_SCALE / (layers * slabs * members)
    table = jnp.concatenate([table_extinction[None] * scale, table_colour], axis=0)
    table = jnp.pad(table, ((0, 0), (0, LANES - table.shape[1])))
    table = jnp.broadcast_to(table[:, None, :], (4, 8, LANES))

    def cut(array, j, axis):
        return lax.dynamic_slice_in_dim(array, j * rows, rows, axis=axis)

    own = [to_chip(cut(fluid_state, chip ^ d, 2), d) for d in range(chips)]

    theirs = to_core(material)
    both = jnp.stack([jnp.where(upper == 1, theirs, material), jnp.where(upper == 1, material, theirs)])
    kinds = [cut(both, chip, 2)]
    for d in range(1, chips):
        pairs = [(2 * k, 2 * (k ^ d) + k // half) for k in range(chips)]
        kinds.append(lax.ppermute(cut(both, chip ^ d, 2), "swap", pairs))

    block = (layers, rows, width)
    cells = layers * rows * width
    other, outer = call(functools.partial(route_kernel, chips), own, [((half, 2, *block), F32), ((2, *block), F32)])
    *kinds, _ = lax.optimization_barrier((*kinds, outer))
    other = to_core(other)
    ring = []
    for z in range(slabs):
        for w in range(members):
            to = ((z + 1) % slabs, w - 1) if w % 2 else ((z - 1) % slabs, w + 1)
            ring.append((z * members + w, to[0] * members + to[1]))
    far = lax.ppermute(outer, ("slab", "swap"), ring)

    deep = (chips * layers, rows, width)
    dense, image, edge, edge_kind = call(
        functools.partial(inner_kernel, chips),
        [*own, *kinds, other, table],
        [(deep, F32), ((4, rows, width), F32), ((2, 2 * layers, rows, width), F32), (block, jnp.int32)],
        [((2, (chips + 1) * layers, rows, width), F32), (deep, jnp.int32)],
        chips * cells,
    )
    keep, give, tile = call(
        functools.partial(outer_kernel, chips),
        [far, edge, edge_kind, table, dense, image],
        [((half, *block), F32), ((half * layers + 2, rows, width), F32), ((4, rows // 2, width), F32)],
        [(block, F32), ((4, rows, width), F32)],
        cells,
    )
    got = to_core(give)

    kept = [keep[i] for i in range(half)]
    gotten = [got[i * layers : (i + 1) * layers] for i in range(half)]
    chunks = []
    for d in range(chips):
        k = chip ^ d
        back = jnp.where(k // half == upper, pick(kept, k % half), pick(gotten, k % half))
        chunks.append(to_chip(back, d))
    density = jnp.concatenate([pick(chunks, chip ^ j) for j in range(chips)], axis=1)

    partner = got[half * layers :].reshape(4, rows // 2, width)
    tile = over(jnp.where(upper == 1, partner, tile), jnp.where(upper == 1, tile, partner))
    for bit in range(slabs.bit_length() - 1):
        partner = lax.ppermute(tile, "slab", swap_pairs(slabs, 1 << bit))
        behind = slab >> bit & 1
        tile = over(jnp.where(behind == 1, partner, tile), jnp.where(behind == 1, tile, partner))
    rendered = jnp.concatenate([tile[:3], 1.0 - tile[3:4]], axis=0).reshape(4, height * width // members)
    return density, rendered


def solution(mesh):
    return jax.shard_map(
        per_device,
        mesh=mesh,
        in_specs=(P(None, ("slab", "swap"), None, None), P(("slab", "swap"), None, None), P(), P()),
        out_specs=(P(("slab", "swap"), None, None), P(None, "swap")),
        check_vma=False,
    )
```

```python
import functools

import jax
import jax.numpy as jnp
from jax import lax
from jax.experimental import pallas as pl
from jax.experimental.pallas import tpu as pltpu
from jax.sharding import PartitionSpec as P

COURANT = 0.4
DEPTH_SCALE = 2.5
LANES = 128
F32 = jnp.float32
GRANT = 12 << 20
VMEM = pl.BlockSpec(memory_space=pltpu.VMEM)


def swap_pairs(members, mask):
    return [(w, w ^ mask) for w in range(members)]


def pick(arrays, index):
    out = arrays[0]
    for number in range(1, len(arrays)):
        out = jnp.where(index == number, arrays[number], out)
    return out


def advance(state, stage, density, momentum, emit):
    if stage == 4:
        emit(density)
        return
    last = stage == 3
    velocity = momentum / density
    speed = jnp.abs(velocity) + 1.0
    pressure = None if last else momentum * velocity + density
    held = state[stage]
    if held is None:
        state[stage] = (density, momentum, speed, pressure, None, None)
        return
    density0, momentum0, speed0, pressure0, mass0, force0 = held
    face = jnp.maximum(speed0, speed)
    mass = (momentum0 + momentum) - face * (density - density0)
    force = None if last else (pressure0 + pressure) - face * (momentum - momentum0)
    state[stage] = (density, momentum, speed, pressure, mass, force)
    if mass0 is None:
        return
    density1 = density0 - (0.5 * COURANT) * (mass - mass0)
    momentum1 = None if last else momentum0 - (0.5 * COURANT) * (force - force0)
    advance(state, stage + 1, density1, momentum1, emit)


def sweep_tiles(rows, columns, layers, count, backwards, load, dense_at, dense, kind_at, kind, table, finish):
    tall = min(8, rows)
    across = columns // LANES

    def tile(number, carry):
        row = pl.ds(pl.multiple_of(number // across * tall, tall), tall)
        column = pl.ds(pl.multiple_of(number % across * LANES, LANES), LANES)

        def block(state, light, position):
            for layer in range(layers):
                at = position * layers + layer

                def emit(density):
                    own = at - 2 * layers
                    dense[dense_at(own), row, column] = density
                    which = kind[kind_at(own), row, column]
                    factor, red, green, blue = (
                        jnp.take_along_axis(table[n, :tall, :], which, axis=1) for n in range(4)
                    )
                    through = jnp.exp(-(factor * density))
                    hidden = 1.0 - through
                    weight = jnp.where(backwards, hidden, hidden * light[0])
                    keep = jnp.where(backwards, through, 1.0)
                    light[0] = light[0] * through
                    light[1] = light[1] * keep + weight * red
                    light[2] = light[2] * keep + weight * green
                    light[3] = light[3] * keep + weight * blue

                advance(state, 0, *load(at, row, column), emit)

        state = [None] * 4
        zero = jnp.zeros((tall, LANES), F32)
        light = [zero + 1.0, zero, zero, zero]
        block(state, light, 0)
        block(state, light, 1)
        if count <= 5:
            for position in range(2, count):
                block(state, light, position)
        else:

            def step(position, carry):
                state, light = [list(part) for part in carry]
                block(state, light, position)
                return state, light

            state, light = lax.fori_loop(2, count, step, (state, light))
        finish(light, row, column)
        return carry

    lax.fori_loop(0, rows // tall * across, tile, 0)


def inner_kernel(chips, *refs):
    own, kinds = refs[:chips], refs[chips : 2 * chips]
    other, table, keep, give, image, edge, edge_kind, fluid, kind, dense = refs[2 * chips :]
    member = lax.axis_index("swap")
    chip, upper = member // 2, member % 2
    half = chips // 2
    _, layers, rows, columns = own[0].shape
    for d in range(chips):
        k = chip ^ d

        @pl.when(k // half == upper)
        def _():
            at = 2 * (k - upper * half)
            fluid[:, pl.ds((at + 2 * upper) * layers, layers)] = own[d][...]
            kind[pl.ds(at * layers, 2 * layers)] = kinds[d][...].reshape(2 * layers, rows, columns)

        @pl.when(k == jnp.where(upper == 1, half - 1, half))
        def _():
            at = jnp.where(upper == 1, 0, chips)
            fluid[:, pl.ds(at * layers, layers)] = own[d][...]

    for i in range(half):
        fluid[:, pl.ds((2 * i + 1) * layers, layers)] = other[i]

    total = (chips + 1) * layers
    sign = jnp.where(upper == 1, 1.0, -1.0)

    def load(at, row, column):
        at = jnp.where(upper == 1, at, total - 1 - at)
        return fluid[0, at, row, column], sign * fluid[1, at, row, column]

    def place(own):
        return jnp.where(upper == 1, own, chips * layers - 1 - own)

    def finish(light, row, column):
        for n in range(4):
            image[n, row, column] = light[n]

    sweep_tiles(rows, columns, layers, chips + 1, upper == 0, load, place, dense, place, kind, table, finish)
    start = jnp.where(upper == 1, chips - 1, 0) * layers
    edge[...] = fluid[:, pl.ds(start, 2 * layers)]
    edge_kind[...] = kind[pl.ds(start, layers)]
    for i in range(half):
        keep[i] = dense[pl.ds((2 * i + upper) * layers, layers)]
        give[i] = dense[pl.ds((2 * i + 1 - upper) * layers, layers)]


def outer_kernel(far, edge, edge_kind, table, image, last, tile, given, drawn):
    upper = lax.axis_index("swap") % 2
    _, layers, rows, columns = far.shape
    sign = jnp.where(upper == 1, -1.0, 1.0)

    def load(at, row, column):
        source, base, size = (far, at, layers) if at < layers else (edge, at - layers, 2 * layers)
        base = jnp.where(upper == 1, size - 1 - base, base)
        return source[0, base, row, column], sign * source[1, base, row, column]

    def place(own):
        return jnp.where(upper == 1, layers - 1 - own, own)

    def finish(light, row, column):
        inner = [image[n, row, column] for n in range(4)]
        front = [jnp.where(upper == 1, a, b) for a, b in zip(inner, light)]
        back = [jnp.where(upper == 1, b, a) for a, b in zip(inner, light)]
        drawn[3, row, column] = front[0] * back[0]
        for n in range(1, 4):
            drawn[n - 1, row, column] = front[n] + front[0] * back[n]

    sweep_tiles(rows, columns, layers, 3, upper == 1, load, place, last, place, edge_kind, table, finish)
    short = rows // 2
    for n in range(4):
        low, high = drawn[n, :short], drawn[n, short:]
        tile[n] = jnp.where(upper == 1, high, low)
        given[n] = jnp.where(upper == 1, low, high)


def route_kernel(chips, *refs):
    own, (other, outer) = refs[:chips], refs[chips:]
    member = lax.axis_index("swap")
    chip, upper = member // 2, member % 2
    half = chips // 2
    for d in range(chips):
        k = chip ^ d

        @pl.when(k // half != upper)
        def _():
            other[k - (1 - upper) * half] = own[d][...]

        @pl.when(k == upper * (chips - 1))
        def _():
            outer[...] = own[d][...]


def call(kernel, operands, outs, scratch=(), cells=0):
    return pl.pallas_call(
        kernel,
        out_shape=[jax.ShapeDtypeStruct(shape, dtype) for shape, dtype in outs],
        in_specs=[VMEM] * len(operands),
        out_specs=[VMEM] * len(outs),
        scratch_shapes=[pltpu.VMEM(shape, dtype) for shape, dtype in scratch],
        compiler_params=pltpu.CompilerParams(vmem_limit_bytes=GRANT),
        cost_estimate=pl.CostEstimate(flops=300 * cells, bytes_accessed=16 * cells, transcendentals=6 * cells),
    )(*operands)


def over(nearer, farther):
    return jnp.concatenate([nearer[:3] + nearer[3:4] * farther[:3], nearer[3:4] * farther[3:4]], axis=0)


def per_device(fluid_state, material, table_colour, table_extinction):
    slabs = lax.axis_size("slab")
    members = lax.axis_size("swap")
    chips = members // 2
    half = chips // 2
    member = lax.axis_index("swap")
    slab = lax.axis_index("slab")
    chip, upper = member // 2, member % 2
    _, layers, height, width = fluid_state.shape
    rows = height // chips

    def to_chip(block, d):
        if d == 0:
            return block
        return lax.ppermute(block, "swap", swap_pairs(members, 2 * d))

    def to_core(block):
        return lax.ppermute(block, "swap", swap_pairs(members, 1))

    scale = DEPTH_SCALE / (layers * slabs * members)
    table = jnp.concatenate([table_extinction[None] * scale, table_colour], axis=0)
    table = jnp.pad(table, ((0, 0), (0, LANES - table.shape[1])))
    table = jnp.broadcast_to(table[:, None, :], (4, 8, LANES))

    def cut(array, j, axis):
        return lax.dynamic_slice_in_dim(array, j * rows, rows, axis=axis)

    own, uncut = [None] * chips, fluid_state
    for d in [*range(1, chips), 0]:
        piece = cut(uncut, chip ^ d, 2)
        own[d] = to_chip(piece, d)
        uncut, _ = lax.optimization_barrier((uncut, piece))

    theirs = to_core(material)
    both = jnp.stack([jnp.where(upper == 1, theirs, material), jnp.where(upper == 1, material, theirs)])
    kinds = [cut(both, chip, 2)]
    for d in range(1, chips):
        pairs = [(2 * k, 2 * (k ^ d) + k // half) for k in range(chips)]
        kinds.append(lax.ppermute(cut(both, chip ^ d, 2), "swap", pairs))

    block = (layers, rows, width)
    cells = layers * rows * width
    other, outer = call(functools.partial(route_kernel, chips), own, [((half, 2, *block), F32), ((2, *block), F32)])
    *kinds, _ = lax.optimization_barrier((*kinds, outer))
    other = to_core(other)
    ring = []
    for z in range(slabs):
        for w in range(members):
            to = ((z + 1) % slabs, w - 1) if w % 2 else ((z - 1) % slabs, w + 1)
            ring.append((z * members + w, to[0] * members + to[1]))
    far = lax.ppermute(outer, ("slab", "swap"), ring)

    deep = (chips * layers, rows, width)
    keep, give, image, edge, edge_kind = call(
        functools.partial(inner_kernel, chips),
        [*own, *kinds, other, table],
        [((half, *block), F32)] * 2
        + [((4, rows, width), F32), ((2, 2 * layers, rows, width), F32), (block, jnp.int32)],
        [((2, (chips + 1) * layers, rows, width), F32), (deep, jnp.int32), (deep, F32)],
        chips * cells,
    )
    got = to_core(give)
    short = (4, rows // 2, width)
    last, tile, given = call(
        outer_kernel,
        [far, edge, edge_kind, table, image],
        [(block, F32), (short, F32), (short, F32)],
        [((4, rows, width), F32)],
        cells,
    )
    partner = to_core(given)

    kept = [jnp.where(i == upper * (half - 1), last, keep[i]) for i in range(half)]
    gotten = [got[i] for i in range(half)]
    chunks = []
    for d in range(chips):
        k = chip ^ d
        back = jnp.where(k // half == upper, pick(kept, k % half), pick(gotten, k % half))
        chunks.append(to_chip(back, d))
    density = jnp.concatenate([pick(chunks, chip ^ j) for j in range(chips)], axis=1)

    tile = over(jnp.where(upper == 1, partner, tile), jnp.where(upper == 1, tile, partner))
    for bit in range(slabs.bit_length() - 1):
        partner = lax.ppermute(tile, "slab", swap_pairs(slabs, 1 << bit))
        behind = slab >> bit & 1
        tile = over(jnp.where(behind == 1, partner, tile), jnp.where(behind == 1, tile, partner))
    rendered = jnp.concatenate([tile[:3], 1.0 - tile[3:4]], axis=0).reshape(4, height * width // members)
    return density, rendered


def solution(mesh):
    return jax.shard_map(
        per_device,
        mesh=mesh,
        in_specs=(P(None, ("slab", "swap"), None, None), P(("slab", "swap"), None, None), P(), P()),
        out_specs=(P(("slab", "swap"), None, None), P(None, "swap")),
        check_vma=False,
    )
```
